16 devices in a mesh: dp: 2 (over y, z), fsdp: 8 (over x, core).
Axes of the slice: x: 4, y: 2, z: 1, core: 2. Of those that a mesh axis runs over, the one named last changes fastest.
The devices are a block of a 4x4x8 slice.
Arguments:
- x: bfloat16 [16, 1024, 2048], P(('dp', 'fsdp')), parts along dimension 0
- gain: bfloat16 [2, 2048], replicated
- w_in: bfloat16 [2, 2048, 18944], P(None, None, 'fsdp')
- w_out: bfloat16 [2, 10240, 2048], P(None, 'fsdp')
Outputs:
- output 1: bfloat16 [16, 1024, 2048], P(('dp', 'fsdp')), parts along dimension 0
- output 2: bfloat16 [2, 16, 1024, 256], P(None, ('dp', 'fsdp')), parts along dimension 1
- output 3: bfloat16 [2, 16, 1024, 256], P(None, ('dp', 'fsdp')), parts along dimension 1
There are 2 independent parts. The reference program is written for one: setup_inputs(seed, part) draws one part's arguments, and reference() takes and returns one part's arrays. A program takes and returns all parts, laid end to end along the dimension named above; an argument that names none is the same for every part.
All inputs are finite; a program needn't handle non-finite values.
Results may differ from the reference program's by a relative error of at most 0.012933.
Values are sent between devices in bfloat16 or wider.
A program may use at most 768 MiB of HBM per device.

```python
import jax
import jax.numpy as jnp
from jax import lax

BATCH_SEQS = 8
SEQ_LEN = 1024
D_MODEL = 2048
NUM_HEADS = 8
FF_DIM = 8192
HEAD_DIM = 256
NUM_LAYERS = 2
Q_COLS = NUM_HEADS * HEAD_DIM
IN_COLS = Q_COLS + 2 * HEAD_DIM + 2 * FF_DIM
OUT_ROWS = Q_COLS + FF_DIM
ROPE_BASE = 10000.0
NORM_EPS = 1e-6


def normal_weight(key, rows, cols):
    return (jax.random.normal(key, (rows, cols), jnp.float32) * rows ** -0.5).astype(jnp.bfloat16)


def setup_inputs(seed: int = 0, part: int = 0) -> dict:
    key = jax.random.key(seed)
    act_key = jax.random.fold_in(jax.random.fold_in(key, 1), part)
    gain_key, in_key, out_key = jax.random.split(jax.random.fold_in(key, 2), 3)
    in_keys = jax.random.split(in_key, NUM_LAYERS)
    out_keys = jax.random.split(out_key, NUM_LAYERS)
    x = (0.5 * jax.random.normal(act_key, (BATCH_SEQS, SEQ_LEN, D_MODEL), jnp.float32)).astype(jnp.bfloat16)
    gain = (1.0 + 0.3 * jax.random.normal(gain_key, (NUM_LAYERS, D_MODEL), jnp.float32)).astype(jnp.bfloat16)
    w_in = jnp.stack([normal_weight(in_keys[layer], D_MODEL, IN_COLS) for layer in range(NUM_LAYERS)])
    w_out = jnp.stack([normal_weight(out_keys[layer], OUT_ROWS, D_MODEL) for layer in range(NUM_LAYERS)])
    return {"x": x, "gain": gain, "w_in": w_in, "w_out": w_out}


def rope_tables():
    half_dim = HEAD_DIM // 2
    inv_freq = ROPE_BASE ** (-jnp.arange(half_dim, dtype=jnp.float32) / half_dim)
    angle = jnp.arange(SEQ_LEN, dtype=jnp.float32)[:, None] * inv_freq[None, :]
    return jnp.cos(angle), jnp.sin(angle)


def apply_rope(tensor, cos_table, sin_table):
    half_dim = HEAD_DIM // 2
    first = tensor[..., :half_dim]
    second = tensor[..., half_dim:]
    return jnp.concatenate([first * cos_table - second * sin_table, second * cos_table + first * sin_table], axis=-1)


def layer_norm(hidden, gain_vec):
    x_float = hidden.astype(jnp.float32)
    centred = x_float - jnp.mean(x_float, axis=-1, keepdims=True)
    variance = jnp.mean(centred * centred, axis=-1, keepdims=True)
    return (centred * lax.rsqrt(variance + NORM_EPS) * gain_vec.astype(jnp.float32)).astype(jnp.bfloat16)


def layer_step(hidden, layer_weights):
    gain_vec, w_in_layer, w_out_layer = layer_weights
    normed = layer_norm(hidden, gain_vec)
    projected = jnp.dot(normed, w_in_layer, preferred_element_type=jnp.float32).astype(jnp.bfloat16)
    query = projected[:, :Q_COLS].reshape(SEQ_LEN, NUM_HEADS, HEAD_DIM)
    key_raw = projected[:, Q_COLS:Q_COLS + HEAD_DIM]
    value = projected[:, Q_COLS + HEAD_DIM:Q_COLS + 2 * HEAD_DIM]
    gate = projected[:, Q_COLS + 2 * HEAD_DIM:Q_COLS + 2 * HEAD_DIM + FF_DIM]
    up_proj = projected[:, Q_COLS + 2 * HEAD_DIM + FF_DIM:]
    cos_table, sin_table = rope_tables()
    q_rot = (apply_rope(query.astype(jnp.float32), cos_table[:, None, :], sin_table[:, None, :]) * HEAD_DIM ** -0.5).astype(jnp.bfloat16)
    k_rot = apply_rope(key_raw.astype(jnp.float32), cos_table, sin_table).astype(jnp.bfloat16)
    scores = jnp.einsum("qhd,kd->qhk", q_rot.astype(jnp.float32), k_rot.astype(jnp.float32))
    causal = jnp.arange(SEQ_LEN)[:, None, None] >= jnp.arange(SEQ_LEN)[None, None, :]
    scores = jnp.where(causal, scores, -1e30)
    exp_scores = jnp.exp(scores - jnp.max(scores, axis=-1, keepdims=True))
    row_sum = jnp.sum(exp_scores, axis=-1, keepdims=True)
    attended = jnp.einsum("qhk,kd->qhd", exp_scores.astype(jnp.bfloat16).astype(jnp.float32), value.astype(jnp.float32)) / row_sum
    attended = attended.astype(jnp.bfloat16).reshape(SEQ_LEN, Q_COLS)
    gated = (jax.nn.silu(gate.astype(jnp.float32)) * up_proj.astype(jnp.float32)).astype(jnp.bfloat16)
    mixed = jnp.concatenate([attended, gated], axis=-1)
    out_sum = jnp.dot(mixed, w_out_layer, preferred_element_type=jnp.float32)
    new_hidden = (hidden.astype(jnp.float32) + out_sum).astype(jnp.bfloat16)
    return new_hidden, (k_rot, value)


def reference(x, gain, w_in, w_out):
    def run_sequence(seq_x):
        final, caches = lax.scan(layer_step, seq_x, (gain, w_in, w_out))
        return final, caches[0], caches[1]
    hidden, key_cache, value_cache = lax.map(run_sequence, x)
    return hidden, jnp.transpose(key_cache, (1, 0, 2, 3)), jnp.transpose(value_cache, (1, 0, 2, 3))
```

```python
import functools

import jax
import jax.numpy as jnp
import numpy as np
from jax import lax
from jax.experimental import pallas as pl
from jax.experimental.pallas import tpu as pltpu
from jax.sharding import PartitionSpec as P

HEAD_DIM = 256
ROPE_BASE = 10000.0
NORM_EPS = 1e-6
MESH = pl.DeviceIdType.MESH
TILE = 512
ROWS = 512
CHUNKS = 4
AHEAD = 4


def rope_tables(seq_len):
    half = HEAD_DIM // 2
    angle = np.arange(seq_len)[:, None] * ROPE_BASE ** (-np.arange(half) / half)
    return np.cos(angle).astype(np.float32), np.sin(angle).astype(np.float32)


def part_rows(rows):
    step = 8 * CHUNKS
    outer = rows // (3 * step) * step
    return outer, rows - 2 * outer


def aligned(value, step):
    return pl.multiple_of(value, step)


def loop(lo, hi, body):
    lax.fori_loop(lo, hi, lambda i, c: (body(i), c)[1], 0)


def kernel(
    groups, group, x_ref, gain_ref, cos_ref, sin_ref, w_in_ref, w_out_ref,
    y_ref, k_ref, v_ref, g_in, g_out,
    h, acc, proj, kbuf, vbuf, wbuf, wtail,
    rx, rm, rp, rd, send, sd, wsem, tsem, ysem, kvsem,
):
    layers, width, cols = w_in_ref.shape
    out_rows = w_out_ref.shape[1]
    seq = x_ref.shape[1]
    rows_total = out_rows * group
    ff = cols * group - rows_total - 2 * HEAD_DIM
    q_cols = rows_total - ff
    heads = q_cols // HEAD_DIM
    chips = group // 2
    n_full = cols // TILE
    tail = cols - n_full * TILE
    half = HEAD_DIM // 2
    items = 3 * CHUNKS
    total = items * 2 * layers

    dp = lax.axis_index("dp")
    me = lax.axis_index("fsdp")
    chip, core = lax.div(me, 2), lax.rem(me, 2)
    side = lax.rem(dp, 2)

    def dev(chip_off, other_core=0):
        c = core if isinstance(other_core, int) and other_core == 0 else lax.rem(core + other_core, 2)
        return 2 * lax.rem(chip + chip_off + chips, chips) + c

    right, left, far = dev(1), dev(-1), dev(2)
    sib = 2 * chip + (1 - core)
    to_right, to_left = {"dp": dp, "fsdp": right}, {"dp": dp, "fsdp": left}
    to_pair = {"dp": dp + 1 - 2 * side, "fsdp": me}
    to_sib = {"dp": dp, "fsdp": sib}

    barrier = pltpu.get_barrier_semaphore()
    for target in (to_right, to_left, to_pair, to_sib):
        pl.semaphore_signal(barrier, inc=1, device_id=target, device_id_type=MESH)
    pl.semaphore_wait(barrier, 4)

    kinds = []
    for own, land, rows in ((w_in_ref, g_in, width), (w_out_ref, g_out, out_rows)):
        outer, middle = part_rows(rows)
        kinds.append((own, land, outer, middle))

    def region(kind, part, k, chunks=1):
        _, _, outer, middle = kinds[kind]
        if part == 1:
            rows = middle // CHUNKS
            return aligned(outer + k * rows, 8), rows * chunks
        rows = outer // CHUNKS
        where = side if part == 0 else 1 - side
        return aligned(where * (outer + middle) + k * rows, 8), rows * chunks

    def remote(kind, src, slot, layer, off, rows, ssem, rsem, target):
        _, land, _, _ = kinds[kind]
        source = src.at[layer] if slot is None else src.at[layer, slot]
        return pltpu.make_async_remote_copy(
            src_ref=source.at[pl.ds(off, rows)],
            dst_ref=land.at[layer, me if slot is None else slot, pl.ds(off, rows)],
            send_sem=ssem, recv_sem=rsem, device_id=target, device_id_type=MESH,
        )

    def arrival(kind, layer, slot, off, rows, rsem):
        _, land, _, _ = kinds[kind]
        ref = land.at[layer, slot, pl.ds(off, rows)]
        return pltpu.make_async_remote_copy(
            src_ref=ref, dst_ref=ref, send_sem=sd.at[0], recv_sem=rsem,
            device_id=to_sib, device_id_type=MESH,
        )

    def send_x(g):
        w, i = lax.div(g, items), lax.rem(g, items)
        layer = lax.div(w, 2)
        k = lax.rem(i, CHUNKS)
        for kind in range(2):
            own, land, _, _ = kinds[kind]

            @pl.when(lax.rem(w, 2) == kind)
            def _():
                for stage in range(3):
                    @pl.when(lax.div(i, CHUNKS) == stage)
                    def _():
                        for way, (target, rsem) in enumerate(((to_right, rx), (to_left, rm))):
                            ssem = send.at[w, 3 * way + stage]
                            if stage < 2:
                                off, rows = region(kind, stage, k)
                                remote(kind, own, None, layer, off, rows, ssem, rsem.at[g], target).start()
                            else:
                                off, rows = region(kind, way, k)
                                slot = left if way == 0 else right
                                remote(kind, land, slot, layer, off, rows, ssem, rsem.at[g], target).start()

    def tick(g):
        w, i = lax.div(g, items), lax.rem(g, items)
        layer = lax.div(w, 2)
        k = lax.rem(i, CHUNKS)
        for kind in range(2):
            _, land, _, _ = kinds[kind]

            @pl.when(lax.rem(w, 2) == kind)
            def _():
                for stage in range(3):
                    @pl.when(lax.div(i, CHUNKS) == stage)
                    def _():
                        for way, rsem in enumerate((rx, rm)):
                            slot = far if stage == 2 else (left if way == 0 else right)
                            off, rows = region(kind, way if stage == 2 else stage, k)
                            arrival(kind, layer, slot, off, rows, rsem.at[g]).wait_recv()
                        off, rows = region(kind, 0, k)
                        if stage == 0:
                            for n, slot in enumerate((left, right)):
                                remote(kind, land, slot, layer, off, rows, send.at[w, 6 + n], rp.at[w, n], to_pair).start()
                        if stage == 2:
                            remote(kind, land, far, layer, off, rows, send.at[w, 8], rp.at[w, 2], to_pair).start()

        @pl.when(g + AHEAD < total)
        def _():
            send_x(g + AHEAD)

    def ticks(lo, hi):
        loop(jnp.minimum(lo, total), jnp.minimum(hi, total), tick)

    def take_pair(kind, layer, n):
        off, rows = region(kind, 2, 0, CHUNKS)
        slot = (left, right, far)[n]
        arrival(kind, layer, slot, off, rows, rp.at[2 * layer + kind, n]).wait_recv()

    def sib_send(kind, layer, n):
        own, land, outer, middle = kinds[kind]
        w = 2 * layer + kind
        src, slot = (own, None) if n == 0 else (land, (None, left, right, far)[n])
        remote(kind, src, slot, layer, 0, 2 * outer + middle, sd.at[w, n], rd.at[w, n], to_sib).start()

    def sib_slot(n):
        return (sib, dev(-1, 1), dev(1, 1), dev(2, 1))[n]

    def take_sib(kind, layer, n):
        _, _, outer, middle = kinds[kind]
        ref = kinds[kind][1].at[layer, sib_slot(n)]
        pltpu.make_async_remote_copy(
            src_ref=ref, dst_ref=ref, send_sem=sd.at[2 * layer + kind, n], recv_sem=rd.at[2 * layer + kind, n],
            device_id=to_sib, device_id_type=MESH,
        ).wait_recv()

    def shard_at(s):
        off = jnp.where(s < 2, 0, jnp.where(s >= 6, 2, jnp.where(lax.rem(s, 2) == 0, -1, 1)))
        flip = jnp.where((s == 1) | (s == 4) | (s == 5) | (s == 7), 1, 0)
        return 2 * lax.rem(chip + off + chips, chips) + lax.rem(core + flip, 2)

    def normalise(layer):
        gain = gain_ref[layer].astype(jnp.float32)

        def block(b):
            rows = pl.ds(aligned(b * 128, 128), 128)
            hidden = acc[rows, :].astype(jnp.bfloat16).astype(jnp.float32)
            acc[rows, :] = hidden
            centred = hidden - jnp.mean(hidden, axis=-1, keepdims=True)
            variance = jnp.mean(centred * centred, axis=-1, keepdims=True)
            h[rows, :] = (centred * lax.rsqrt(variance + NORM_EPS) * gain).astype(jnp.bfloat16)

        loop(0, seq // 128, block)

    def in_shard(layer, s):
        d = shard_at(s)
        odd = lax.rem(d, 2)
        base = d * cols - odd * (cols % 128)

        def fetch(j, slot):
            window = pl.ds(aligned(j * TILE, TILE), TILE)

            @pl.when(s == 0)
            def _():
                pltpu.make_async_copy(w_in_ref.at[layer, :, window], wbuf.at[slot], wsem.at[slot]).start()

            @pl.when(s > 0)
            def _():
                pltpu.make_async_copy(g_in.at[layer, d, :, window], wbuf.at[slot], wsem.at[slot]).start()

        tail_window = pl.ds(n_full * TILE, tail)

        @pl.when(s == 0)
        def _():
            pltpu.make_async_copy(w_in_ref.at[layer, :, tail_window], wtail, tsem).start()

        @pl.when(s > 0)
        def _():
            pltpu.make_async_copy(g_in.at[layer, d, :, tail_window], wtail, tsem).start()

        def multiply(weights, n, col):
            shift = cols % 128
            padded = -(-(n + shift) // 128) * 128

            def block(b):
                rows = pl.ds(aligned(b * ROWS, ROWS), ROWS)
                out = jnp.dot(h[rows, :], weights[...], preferred_element_type=jnp.float32).astype(jnp.bfloat16)

                @pl.when(odd == 0)
                def _():
                    proj.at[rows, pl.ds(aligned(base + col, 128), -(-n // 128) * 128)][:, :n] = out

                @pl.when(odd == 1)
                def _():
                    proj.at[rows, pl.ds(aligned(base + col, 128), padded)][:, shift:shift + n] = out

            loop(0, seq // ROWS, block)

        fetch(0, 0)

        def full(j):
            slot = lax.rem(j, 2)

            @pl.when(j + 1 < n_full)
            def _():
                fetch(j + 1, 1 - slot)

            pltpu.make_async_copy(g_in.at[0, 0, :, pl.ds(0, TILE)], wbuf.at[slot], wsem.at[slot]).wait()
            multiply(wbuf.at[slot], TILE, j * TILE)

        loop(0, n_full, full)
        pltpu.make_async_copy(g_in.at[0, 0, :, tail_window], wtail, tsem).wait()
        multiply(wtail, tail, n_full * TILE)

    def rotate(a, rows):
        cos, sin = cos_ref[rows, :], sin_ref[rows, :]
        first, second = a[:, :half], a[:, half:]
        return jnp.concatenate([first * cos - second * sin, second * cos + first * sin], axis=-1)

    q_block = 256

    def keys(layer):
        def block(b):
            rows = pl.ds(aligned(b * q_block, q_block), q_block)
            key = proj[rows, q_cols:q_cols + HEAD_DIM].astype(jnp.float32)
            kbuf[rows, :] = rotate(key, rows).astype(jnp.bfloat16)
            vbuf[rows, :] = proj[rows, q_cols + HEAD_DIM:q_cols + 2 * HEAD_DIM]

        loop(0, seq // q_block, block)
        pltpu.make_async_copy(kbuf, k_ref.at[layer, 0], kvsem.at[0]).start()
        pltpu.make_async_copy(vbuf, v_ref.at[layer, 0], kvsem.at[1]).start()

    blocks = seq // q_block
    shift_cols = 2 * HEAD_DIM

    def attend(t):
        head = heads - 1 - lax.div(t, blocks)
        b = lax.rem(t, blocks)
        rows = pl.ds(aligned(b * q_block, q_block), q_block)
        q = proj[rows, pl.ds(aligned(head * HEAD_DIM, HEAD_DIM), HEAD_DIM)].astype(jnp.float32)
        q = (rotate(q, rows) * HEAD_DIM ** -0.5).astype(jnp.bfloat16)
        s = lax.dot_general(q, kbuf[...], (((1,), (1,)), ((), ())), preferred_element_type=jnp.float32)
        row = b * q_block + lax.broadcasted_iota(jnp.int32, s.shape, 0)
        s = jnp.where(row >= lax.broadcasted_iota(jnp.int32, s.shape, 1), s, -1e30)
        e = jnp.exp(s - jnp.max(s, axis=-1, keepdims=True))
        o = jnp.dot(e.astype(jnp.bfloat16), vbuf[...], preferred_element_type=jnp.float32)
        o = o / jnp.sum(e, axis=-1, keepdims=True)
        proj[rows, pl.ds(aligned(head * HEAD_DIM + shift_cols, HEAD_DIM), HEAD_DIM)] = o.astype(jnp.bfloat16)

    gate0 = q_cols + 2 * HEAD_DIM
    up0 = gate0 + ff

    def gated(t):
        def block(b):
            rows = pl.ds(aligned(b * 256, 256), 256)
            gate_cols = pl.ds(aligned(gate0 + t * TILE, 128), TILE)
            gate = proj[rows, gate_cols].astype(jnp.float32)
            up = proj[rows, pl.ds(aligned(up0 + t * TILE, 128), TILE)].astype(jnp.float32)
            proj[rows, gate_cols] = (jax.nn.silu(gate) * up).astype(jnp.bfloat16)

        loop(0, seq // 256, block)

    n_out = width // TILE

    def out_shard(layer, s):
        d = shard_at(s)

        def fetch(n, slot):
            window = pl.ds(aligned(n * TILE, TILE), TILE)
            target = wbuf.at[slot, pl.ds(0, out_rows)]

            @pl.when(s == 0)
            def _():
                pltpu.make_async_copy(w_out_ref.at[layer, :, window], target, wsem.at[slot]).start()

            @pl.when(s > 0)
            def _():
                pltpu.make_async_copy(g_out.at[layer, d, :, window], target, wsem.at[slot]).start()

        fetch(0, 0)
        left_cols = pl.ds(aligned(shift_cols + d * out_rows, 128), out_rows)

        def tile(n):
            slot = lax.rem(n, 2)

            @pl.when(n + 1 < n_out)
            def _():
                fetch(n + 1, 1 - slot)

            target = wbuf.at[slot, pl.ds(0, out_rows)]
            pltpu.make_async_copy(g_out.at[0, 0, :, pl.ds(0, TILE)], target, wsem.at[slot]).wait()

            def block(b):
                rows = pl.ds(aligned(b * ROWS, ROWS), ROWS)
                window = pl.ds(aligned(n * TILE, TILE), TILE)
                acc[rows, window] += jnp.dot(
                    proj[rows, left_cols], wbuf[slot, :out_rows, :], preferred_element_type=jnp.float32
                )

            loop(0, seq // ROWS, block)

        loop(0, n_out, tile)

    loop(0, AHEAD, send_x)
    copy = pltpu.make_async_copy(x_ref.at[0], h, ysem)
    copy.start()
    copy.wait()

    def widen(b):
        rows = pl.ds(aligned(b * 128, 128), 128)
        acc[rows, :] = h[rows, :].astype(jnp.float32)

    loop(0, seq // 128, widen)

    def layer_step(layer):
        g0 = 2 * items * layer
        sib_send(0, layer, 0)
        sib_send(1, layer, 0)
        normalise(layer)

        def in_step(s):
            lo = jnp.where(s == 1, 1, jnp.where(s == 2, 2, s + 7))
            hi = jnp.where(s == 0, 1, jnp.where(s == 1, 2, s + 8))
            lo = jnp.where(s == 0, 1, lo)
            ticks(g0 + lo, g0 + hi)

            @pl.when(s == 1)
            def _():
                take_sib(0, layer, 0)

            @pl.when(s == 2)
            def _():
                for n in (0, 1):
                    take_pair(0, layer, n)
                    sib_send(0, layer, n + 1)

            for n in (0, 1, 2):
                @pl.when(s == (4, 5, 7)[n])
                def _():
                    take_sib(0, layer, n + 1)

            @pl.when(s == 6)
            def _():
                take_pair(0, layer, 2)
                sib_send(0, layer, 3)

            in_shard(layer, s)

        loop(0, 8, in_step)
        keys(layer)

        def attend_step(t):
            @pl.when(lax.rem(t, 8) == 0)
            def _():
                ticks(g0 + 15 + lax.div(t, 8), g0 + 16 + lax.div(t, 8))
            attend(t)

        loop(0, heads * blocks, attend_step)

        def gated_step(t):
            @pl.when(lax.rem(t, 8) == 0)
            def _():
                ticks(g0 + 19 + lax.div(t, 8), g0 + 20 + lax.div(t, 8))
            gated(t)

        loop(0, ff // TILE, gated_step)

        def out_step(s):
            lo = jnp.where(s == 0, 21, jnp.where(s == 2, 22, jnp.where(s == 3, 23, 24)))
            hi = jnp.where((s == 0) | (s == 2) | (s == 3) | (s == 6), lo + 1, lo)
            ticks(g0 + lo, g0 + hi)

            @pl.when(s == 1)
            def _():
                take_sib(1, layer, 0)

            @pl.when(s == 2)
            def _():
                for n in (0, 1):
                    take_pair(1, layer, n)
                    sib_send(1, layer, n + 1)

            for n in (0, 1, 2):
                @pl.when(s == (4, 5, 7)[n])
                def _():
                    take_sib(1, layer, n + 1)

            @pl.when(s == 6)
            def _():
                take_pair(1, layer, 2)
                sib_send(1, layer, 3)

            out_shard(layer, s)

        loop(0, 8, out_step)
        pltpu.make_async_copy(kbuf, k_ref.at[layer, 0], kvsem.at[0]).wait()
        pltpu.make_async_copy(vbuf, v_ref.at[layer, 0], kvsem.at[1]).wait()

    tick(0)
    loop(0, layers, layer_step)

    def narrow(b):
        rows = pl.ds(aligned(b * 128, 128), 128)
        h[rows, :] = acc[rows, :].astype(jnp.bfloat16)

    loop(0, seq // 128, narrow)
    copy = pltpu.make_async_copy(h, y_ref.at[0], ysem)
    copy.start()

    def drain(layer):
        for kind in range(2):
            _, land, outer, middle = kinds[kind]
            w = 2 * layer + kind
            for n in range(9):
                rows = middle if n in (1, 4, 5) else outer
                ref = land.at[layer, 0, pl.ds(0, rows)]
                pltpu.make_async_remote_copy(
                    src_ref=ref, dst_ref=ref, send_sem=send.at[w, n], recv_sem=rx.at[0],
                    device_id=to_sib, device_id_type=MESH,
                ).wait_send()
            for n in range(4):
                ref = land.at[layer, 0]
                pltpu.make_async_remote_copy(
                    src_ref=ref, dst_ref=ref, send_sem=sd.at[w, n], recv_sem=rx.at[0],
                    device_id=to_sib, device_id_type=MESH,
                ).wait_send()

    loop(0, layers, drain)
    copy.wait()


def solution(mesh):
    batch_axes = ("dp", "fsdp")
    groups, group = mesh.shape["dp"], mesh.shape["fsdp"]

    def device_program(x, gain, w_in, w_out):
        layers, width, cols = w_in.shape
        out_rows = w_out.shape[1]
        seq = x.shape[1]
        total_cols = cols * group
        tail = cols % TILE
        items = 3 * CHUNKS * 2 * layers
        cos, sin = rope_tables(seq)
        any_spec = pl.BlockSpec(memory_space=pl.ANY)
        vmem_spec = pl.BlockSpec(memory_space=pltpu.VMEM)
        bf16, f32 = jnp.bfloat16, jnp.float32
        dma = pltpu.SemaphoreType.DMA
        out = pl.pallas_call(
            functools.partial(kernel, groups, group),
            out_shape=(
                jax.ShapeDtypeStruct(x.shape, bf16),
                jax.ShapeDtypeStruct((layers, 1, seq, HEAD_DIM), bf16),
                jax.ShapeDtypeStruct((layers, 1, seq, HEAD_DIM), bf16),
                jax.ShapeDtypeStruct((layers, group, width, cols), bf16),
                jax.ShapeDtypeStruct((layers, group, out_rows, width), bf16),
            ),
            in_specs=[any_spec, vmem_spec, vmem_spec, vmem_spec, any_spec, any_spec],
            out_specs=[any_spec] * 5,
            scratch_shapes=[
                pltpu.VMEM((seq, width), bf16),
                pltpu.VMEM((seq, width), f32),
                pltpu.VMEM((seq, total_cols), bf16),
                pltpu.VMEM((seq, HEAD_DIM), bf16),
                pltpu.VMEM((seq, HEAD_DIM), bf16),
                pltpu.VMEM((2, width, TILE), bf16),
                pltpu.VMEM((width, tail), bf16),
                dma((items,)),
                dma((items,)),
                dma((2 * layers, 3)),
                dma((2 * layers, 4)),
                dma((2 * layers, 9)),
                dma((2 * layers, 4)),
                dma((2,)),
                dma,
                dma,
                dma((2,)),
            ],
            compiler_params=pltpu.CompilerParams(
                collective_id=0, has_side_effects=True, vmem_limit_bytes=67_043_328
            ),
        )(x, gain.reshape(layers, 1, width), cos, sin, w_in, w_out)
        return out[:3]

    return jax.shard_map(
        device_program,
        mesh=mesh,
        in_specs=(P(batch_axes, None, None), P(None, None), P(None, None, "fsdp"), P(None, "fsdp", None)),
        out_specs=(P(batch_axes, None, None), P(None, batch_axes, None, None), P(None, batch_axes, None, None)),
        check_vma=False,
    )
```

```python
import functools

import jax
import jax.numpy as jnp
import numpy as np
from jax import lax
from jax.experimental import pallas as pl
from jax.experimental.pallas import tpu as pltpu
from jax.sharding import PartitionSpec as P

HEAD_DIM = 256
ROPE_BASE = 10000.0
NORM_EPS = 1e-6
MESH = pl.DeviceIdType.MESH
TILE = 512
CHUNKS = 4
AHEAD = 4


def rope_tables(seq_len):
    half = HEAD_DIM // 2
    angle = np.arange(seq_len)[:, None] * ROPE_BASE ** (-np.arange(half) / half)
    return np.cos(angle).astype(np.float32), np.sin(angle).astype(np.float32)


def part_rows(rows):
    step = 8 * CHUNKS
    outer = round(rows / (3 * step)) * step
    return outer, rows - 2 * outer


def aligned(value, step):
    return pl.multiple_of(value, step)


def loop(lo, hi, body):
    lax.fori_loop(lo, hi, lambda i, c: (body(i), c)[1], 0)


def kernel(
    groups, group, x_ref, gain_ref, cos_ref, sin_ref, w_in_ref, w_out_ref,
    y_ref, k_ref, v_ref, g_in, g_out,
    h, acc, proj, kbuf, vbuf, wbuf, wtail, obuf,
    rx, rm, rp, rd, send, sd, wsem, tsem, ysem, kvsem,
):
    layers, cols, width = w_in_ref.shape
    out_rows = w_out_ref.shape[1]
    seq = x_ref.shape[1]
    rows_total = out_rows * group
    ff = cols * group - rows_total - 2 * HEAD_DIM
    q_cols = rows_total - ff
    heads = q_cols // HEAD_DIM
    chips = group // 2
    n_full = cols // TILE
    rest = (cols - n_full * TILE) // 128 * 128
    edge = cols - n_full * TILE - rest
    half = HEAD_DIM // 2
    items = 3 * CHUNKS
    total = items * 2 * layers

    dp = lax.axis_index("dp")
    me = lax.axis_index("fsdp")
    chip, core = lax.div(me, 2), lax.rem(me, 2)
    side = lax.rem(dp, 2)

    def dev(chip_off, other_core=0):
        c = core if isinstance(other_core, int) and other_core == 0 else lax.rem(core + other_core, 2)
        return 2 * lax.rem(chip + chip_off + chips, chips) + c

    right, left, far = dev(1), dev(-1), dev(2)
    sib = 2 * chip + (1 - core)
    to_right, to_left = {"dp": dp, "fsdp": right}, {"dp": dp, "fsdp": left}
    to_pair = {"dp": dp + 1 - 2 * side, "fsdp": me}
    to_sib = {"dp": dp, "fsdp": sib}

    barrier = pltpu.get_barrier_semaphore()
    for target in (to_right, to_left, to_pair, to_sib):
        pl.semaphore_signal(barrier, inc=1, device_id=target, device_id_type=MESH)
    pl.semaphore_wait(barrier, 4)

    kinds = []
    for own, land, rows in ((w_in_ref, g_in, cols), (w_out_ref, g_out, out_rows)):
        outer, middle = part_rows(rows)
        kinds.append((own, land, outer, middle))

    def part_at(kind, part):
        _, _, outer, middle = kinds[kind]
        if part == 1:
            return outer, middle
        where = side if part == 0 else 1 - side
        return where * (outer + middle), outer

    def region(kind, part, k):
        start, rows = part_at(kind, part)
        return aligned(start + k * (rows // CHUNKS), 8), rows // CHUNKS

    def remote(kind, src, slot, layer, off, rows, ssem, rsem, target):
        _, land, _, _ = kinds[kind]
        source = src.at[layer] if slot is None else src.at[layer, slot]
        return pltpu.make_async_remote_copy(
            src_ref=source.at[pl.ds(off, rows)],
            dst_ref=land.at[layer, me if slot is None else slot, pl.ds(off, rows)],
            send_sem=ssem, recv_sem=rsem, device_id=target, device_id_type=MESH,
        )

    def arrival(kind, layer, slot, off, rows, rsem):
        _, land, _, _ = kinds[kind]
        ref = land.at[layer, slot, pl.ds(off, rows)]
        return pltpu.make_async_remote_copy(
            src_ref=ref, dst_ref=ref, send_sem=sd.at[0], recv_sem=rsem,
            device_id=to_sib, device_id_type=MESH,
        )

    def send_x(g):
        w, i = lax.div(g, items), lax.rem(g, items)
        layer = lax.div(w, 2)
        k = lax.rem(i, CHUNKS)
        for kind in range(2):
            own, land, _, _ = kinds[kind]

            @pl.when(lax.rem(w, 2) == kind)
            def _():
                for stage in range(3):
                    @pl.when((lax.div(i, CHUNKS) == stage))
                    def _():
                        for way, (target, rsem) in enumerate(((to_right, rx), (to_left, rm))):
                            ssem = send.at[w, 3 * way + stage]
                            if stage < 2:
                                off, rows = region(kind, stage, k)
                                remote(kind, own, None, layer, off, rows, ssem, rsem.at[g], target).start()
                            else:
                                off, rows = region(kind, way, k)
                                slot = left if way == 0 else right
                                remote(kind, land, slot, layer, off, rows, ssem, rsem.at[g], target).start()

    def tick(g):
        w, i = lax.div(g, items), lax.rem(g, items)
        layer = lax.div(w, 2)
        k = lax.rem(i, CHUNKS)
        for kind in range(2):
            _, land, _, _ = kinds[kind]

            @pl.when(lax.rem(w, 2) == kind)
            def _():
                for stage in range(3):
                    @pl.when((lax.div(i, CHUNKS) == stage))
                    def _():
                        for way, rsem in enumerate((rx, rm)):
                            slot = far if stage == 2 else (left if way == 0 else right)
                            off, rows = region(kind, way if stage == 2 else stage, k)
                            arrival(kind, layer, slot, off, rows, rsem.at[g]).wait_recv()
                        off, rows = region(kind, 0, k)
                        if stage == 0:
                            for n, slot in enumerate((left, right)):
                                remote(kind, land, slot, layer, off, rows, send.at[w, 6 + n], rp.at[w, n], to_pair).start()
                        if stage == 2:
                            remote(kind, land, far, layer, off, rows, send.at[w, 8], rp.at[w, 2], to_pair).start()

        @pl.when(g + AHEAD < total)
        def _():
            send_x(g + AHEAD)

    def ticks(lo, hi):
        loop(jnp.minimum(lo, total), jnp.minimum(hi, total), tick)

    def take_pair(kind, layer, n):
        off, rows = part_at(kind, 2)
        off = aligned(off, 8)
        slot = (left, right, far)[n]
        arrival(kind, layer, slot, off, rows, rp.at[2 * layer + kind, n]).wait_recv()

    def sib_rows(kind, n):
        _, _, outer, middle = kinds[kind]
        if n < 3:
            return 0, 2 * outer + middle
        if n == 3:
            return aligned(side * outer, 8), outer + middle
        off, rows = part_at(kind, 2)
        return aligned(off, 8), rows

    def sib_send(kind, layer, n):
        own, land, outer, middle = kinds[kind]
        w = 2 * layer + kind
        src, slot = (own, None) if n == 0 else (land, (None, left, right, far, far)[n])
        off, rows = sib_rows(kind, n)
        remote(kind, src, slot, layer, off, rows, sd.at[w, n], rd.at[w, n], to_sib).start()

    def sib_slot(n):
        return (sib, dev(-1, 1), dev(1, 1), dev(2, 1), dev(2, 1))[n]

    def take_sib(kind, layer, n):
        off, rows = sib_rows(kind, n)
        ref = kinds[kind][1].at[layer, sib_slot(n), pl.ds(off, rows)]
        pltpu.make_async_remote_copy(
            src_ref=ref, dst_ref=ref, send_sem=sd.at[2 * layer + kind, n], recv_sem=rd.at[2 * layer + kind, n],
            device_id=to_sib, device_id_type=MESH,
        ).wait_recv()

    def shard_at(s):
        off = jnp.where(s < 2, 0, jnp.where(s >= 6, 2, jnp.where(lax.rem(s, 2) == 0, -1, 1)))
        flip = jnp.where((s == 1) | (s == 4) | (s == 5) | (s == 7), 1, 0)
        return 2 * lax.rem(chip + off + chips, chips) + lax.rem(core + flip, 2)

    def primed(s):
        return (s == 1) | (s == 3) | (s == 5)

    def normalise(layer):
        gains = gain_ref[...].astype(jnp.float32)
        chosen = lax.broadcasted_iota(jnp.int32, gains.shape, 0) == layer
        gain = jnp.sum(jnp.where(chosen, gains, 0.0), axis=0, keepdims=True)

        def block(b):
            rows = pl.ds(aligned(b * 128, 128), 128)
            hidden = acc[rows, :].astype(jnp.bfloat16).astype(jnp.float32)
            acc[rows, :] = hidden
            centred = hidden - jnp.mean(hidden, axis=-1, keepdims=True)
            variance = jnp.mean(centred * centred, axis=-1, keepdims=True)
            h[rows, :] = (centred * lax.rsqrt(variance + NORM_EPS) * gain).astype(jnp.bfloat16)

        loop(0, seq // 128, block)

    def in_shard(layer, s):
        d = shard_at(s)
        odd = lax.rem(d, 2)
        first = odd * edge
        base = aligned(d * cols + first, 128)

        def fetch(start, rows, target, sem, s=s, d=d):
            @pl.when(s == 0)
            def _():
                pltpu.make_async_copy(w_in_ref.at[layer, pl.ds(aligned(start, 8), rows)], target, sem).start()

            @pl.when(s > 0)
            def _():
                pltpu.make_async_copy(g_in.at[layer, d, pl.ds(aligned(start, 8), rows)], target, sem).start()

        def product(weights):
            return lax.dot_general(
                h[...], weights, (((1,), (1,)), ((), ())), preferred_element_type=jnp.float32
            ).astype(jnp.bfloat16)

        @pl.when(jnp.logical_not(primed(s)))
        def _():
            fetch(first, TILE, wbuf.at[0], wsem.at[0])

        fetch(first + n_full * TILE, rest, wtail.at[pl.ds(0, rest)], tsem.at[0])
        fetch((1 - odd) * (n_full * TILE + rest), edge, wtail.at[pl.ds(rest, edge)], tsem.at[1])

        def full(j):
            slot = lax.rem(j, 2)

            @pl.when(j + 1 < n_full)
            def _():
                fetch(first + (j + 1) * TILE, TILE, wbuf.at[1 - slot], wsem.at[1 - slot])

            @pl.when((j + 1 == n_full) & primed(s + 1))
            def _():
                ahead = shard_at(s + 1)
                fetch(lax.rem(ahead, 2) * edge, TILE, wbuf.at[n_full % 2], wsem.at[n_full % 2], s + 1, ahead)

            pltpu.make_async_copy(g_in.at[0, 0, pl.ds(0, TILE)], wbuf.at[slot], wsem.at[slot]).wait()
            proj[:, pl.ds(aligned(base + j * TILE, 128), TILE)] = product(wbuf[slot])

        loop(0, n_full, full)
        pltpu.make_async_copy(g_in.at[0, 0, pl.ds(0, rest)], wtail.at[pl.ds(0, rest)], tsem.at[0]).wait()
        pltpu.make_async_copy(g_in.at[0, 0, pl.ds(0, edge)], wtail.at[pl.ds(rest, edge)], tsem.at[1]).wait()
        last = product(wtail[...])
        proj[:, pl.ds(aligned(base + n_full * TILE, 128), rest)] = last[:, :rest]
        edges = proj.at[:, pl.ds(aligned(jnp.where(odd == 1, base - 128, base + n_full * TILE + rest), 128), 128)]

        @pl.when(odd == 0)
        def _():
            edges[:, :edge] = last[:, rest:]

        @pl.when(odd == 1)
        def _():
            edges[:, 128 - edge:] = last[:, rest:]

    def rotate(a, rows):
        cos, sin = cos_ref[rows, :], sin_ref[rows, :]
        first, second = a[:, :half], a[:, half:]
        return jnp.concatenate([first * cos - second * sin, second * cos + first * sin], axis=-1)

    q_block = 256

    def keys(layer):
        def block(b):
            rows = pl.ds(aligned(b * q_block, q_block), q_block)
            key = proj[rows, q_cols:q_cols + HEAD_DIM].astype(jnp.float32)
            kbuf[rows, :] = rotate(key, rows).astype(jnp.bfloat16)
            vbuf[rows, :] = proj[rows, q_cols + HEAD_DIM:q_cols + 2 * HEAD_DIM]

        loop(0, seq // q_block, block)
        pltpu.make_async_copy(kbuf, k_ref.at[layer, 0], kvsem.at[0]).start()
        pltpu.make_async_copy(vbuf, v_ref.at[layer, 0], kvsem.at[1]).start()

    blocks = seq // q_block
    shift_cols = 2 * HEAD_DIM

    def attend(t):
        two = heads // 2 - 1 - lax.div(t, blocks)
        b = lax.rem(t, blocks)
        rows = pl.ds(aligned(b * q_block, q_block), q_block)
        q = proj[rows, pl.ds(aligned(two * 2 * HEAD_DIM, 2 * HEAD_DIM), 2 * HEAD_DIM)].astype(jnp.float32)
        q = jnp.concatenate([rotate(q[:, :HEAD_DIM], rows), rotate(q[:, HEAD_DIM:], rows)], axis=0)
        q = (q * HEAD_DIM ** -0.5).astype(jnp.bfloat16)
        for n in range(blocks):
            @pl.when(b == n)
            def _():
                seen = (n + 1) * q_block
                s = lax.dot_general(q, kbuf[:seen, :], (((1,), (1,)), ((), ())), preferred_element_type=jnp.float32)
                own = s[:, n * q_block:]
                row = lax.broadcasted_iota(jnp.int32, own.shape, 0) & (q_block - 1)
                own = jnp.where(row >= lax.broadcasted_iota(jnp.int32, own.shape, 1), own, -1e30)
                s = own if n == 0 else jnp.concatenate([s[:, :n * q_block], own], axis=1)
                e = jnp.exp(s - jnp.max(s, axis=-1, keepdims=True))
                o = jnp.dot(e.astype(jnp.bfloat16), vbuf[:seen, :], preferred_element_type=jnp.float32)
                o = (o / jnp.sum(e, axis=-1, keepdims=True)).astype(jnp.bfloat16)
                place = pl.ds(aligned(two * 2 * HEAD_DIM + shift_cols, 2 * HEAD_DIM), 2 * HEAD_DIM)
                proj[rows, place] = jnp.concatenate([o[:q_block], o[q_block:]], axis=1)

    gate0 = q_cols + 2 * HEAD_DIM
    up0 = gate0 + ff

    def gated(t):
        def block(b):
            rows = pl.ds(aligned(b * 256, 256), 256)
            gate_cols = pl.ds(aligned(gate0 + t * TILE, 128), TILE)
            gate = proj[rows, gate_cols].astype(jnp.float32)
            up = proj[rows, pl.ds(aligned(up0 + t * TILE, 128), TILE)].astype(jnp.float32)
            proj[rows, gate_cols] = (jax.nn.silu(gate) * up).astype(jnp.bfloat16)

        loop(0, seq // 256, block)

    n_out = width // TILE

    def out_shard(layer, s):
        d = shard_at(s)

        def fetch(n, slot, s=s, d=d):
            window = pl.ds(aligned(n * TILE, TILE), TILE)
            target = obuf.at[slot]

            @pl.when(s == 0)
            def _():
                pltpu.make_async_copy(w_out_ref.at[layer, :, window], target, wsem.at[slot]).start()

            @pl.when(s > 0)
            def _():
                pltpu.make_async_copy(g_out.at[layer, d, :, window], target, wsem.at[slot]).start()

        @pl.when(jnp.logical_not(primed(s)))
        def _():
            fetch(0, 0)

        left_cols = pl.ds(aligned(shift_cols + d * out_rows, 128), out_rows)

        def tile(n):
            slot = lax.rem(n, 2)

            @pl.when(n + 1 < n_out)
            def _():
                fetch(n + 1, 1 - slot)

            @pl.when((n + 1 == n_out) & primed(s + 1))
            def _():
                fetch(0, n_out % 2, s + 1, shard_at(s + 1))

            pltpu.make_async_copy(g_out.at[0, 0, :, pl.ds(0, TILE)], obuf.at[slot], wsem.at[slot]).wait()
            window = pl.ds(aligned(n * TILE, TILE), TILE)
            acc[:, window] += jnp.dot(proj[:, left_cols], obuf[slot], preferred_element_type=jnp.float32)

        loop(0, n_out, tile)

    loop(0, AHEAD, send_x)
    copy = pltpu.make_async_copy(x_ref.at[0], h, ysem)
    copy.start()
    copy.wait()

    def widen(b):
        rows = pl.ds(aligned(b * 128, 128), 128)
        acc[rows, :] = h[rows, :].astype(jnp.float32)

    loop(0, seq // 128, widen)

    def layer_step(layer):
        g0 = 2 * items * layer
        sib_send(0, layer, 0)
        sib_send(1, layer, 0)
        normalise(layer)

        def run_ticks(s, start, ends):
            lo, hi = start, ends[0]
            for n in range(1, len(ends)):
                lo = jnp.where(s == n, ends[n - 1], lo)
                hi = jnp.where(s == n, ends[n], hi)
            ticks(g0 + lo, g0 + hi)

        def in_step(s):
            n = 3 * CHUNKS
            ends = (1, 2, 10, 11, 12, 13, 14, 15)
            run_ticks(s, 1, ends)

            @pl.when(s == 0)
            def _():
                take_sib(0, layer, 0)

            @pl.when(s == 2)
            def _():
                for n in (0, 1):
                    take_pair(0, layer, n)
                    sib_send(0, layer, n + 1)

            for first, at in ((1, 4), (3, 7)):
                @pl.when(s == at)
                def _():
                    take_sib(0, layer, first)
                    take_sib(0, layer, first + 1)

            @pl.when(s == 5)
            def _():
                sib_send(0, layer, 3)

            @pl.when(s == 6)
            def _():
                take_pair(0, layer, 2)
                sib_send(0, layer, 4)

            in_shard(layer, s)

        loop(0, 8, in_step)
        keys(layer)

        def attend_step(t):
            @pl.when(lax.rem(t, 4) == 2)
            def _():
                n = g0 + 15 + lax.div(t, 4)
                ticks(n, n + 1)
            attend(t)

        loop(0, heads // 2 * blocks, attend_step)

        def gated_step(t):
            gated(t)

        loop(0, ff // TILE, gated_step)

        def out_step(s):
            n = 6 * CHUNKS
            run_ticks(s, 19, (20, 21, 22, 22, 23, 24, 25, 25))

            @pl.when(s == 0)
            def _():
                take_sib(1, layer, 0)

            @pl.when(s == 2)
            def _():
                for n in (0, 1):
                    take_pair(1, layer, n)
                    sib_send(1, layer, n + 1)

            for first, at in ((1, 4), (3, 7)):
                @pl.when(s == at)
                def _():
                    take_sib(1, layer, first)
                    take_sib(1, layer, first + 1)

            @pl.when(s == 6)
            def _():
                sib_send(1, layer, 3)

            @pl.when(s == 6)
            def _():
                take_pair(1, layer, 2)
                sib_send(1, layer, 4)

            out_shard(layer, s)

        loop(0, 8, out_step)
        pltpu.make_async_copy(kbuf, k_ref.at[layer, 0], kvsem.at[0]).wait()
        pltpu.make_async_copy(vbuf, v_ref.at[layer, 0], kvsem.at[1]).wait()

    tick(0)
    loop(0, layers, layer_step)

    def narrow(b):
        rows = pl.ds(aligned(b * 128, 128), 128)
        h[rows, :] = acc[rows, :].astype(jnp.bfloat16)
        pltpu.make_async_copy(h.at[rows], y_ref.at[0, rows], ysem).start()

    loop(0, seq // 128, narrow)
    copy = pltpu.make_async_copy(h, y_ref.at[0], ysem)

    def drain(layer):
        for kind in range(2):
            _, land, outer, middle = kinds[kind]
            w = 2 * layer + kind
            for n in range(9):
                rows = middle if n in (1, 4, 5) else outer
                ref = land.at[layer, 0, pl.ds(0, rows)]
                pltpu.make_async_remote_copy(
                    src_ref=ref, dst_ref=ref, send_sem=send.at[w, n], recv_sem=rx.at[0],
                    device_id=to_sib, device_id_type=MESH,
                ).wait_send()
            for n in range(5):
                ref = land.at[layer, 0, pl.ds(0, sib_rows(kind, n)[1])]
                pltpu.make_async_remote_copy(
                    src_ref=ref, dst_ref=ref, send_sem=sd.at[w, n], recv_sem=rx.at[0],
                    device_id=to_sib, device_id_type=MESH,
                ).wait_send()

    loop(0, layers, drain)
    copy.wait()


def solution(mesh):
    batch_axes = ("dp", "fsdp")
    groups, group = mesh.shape["dp"], mesh.shape["fsdp"]

    def device_program(x, gain, w_in, w_out):
        w_in = jnp.swapaxes(w_in, 1, 2)
        layers, cols, width = w_in.shape
        out_rows = w_out.shape[1]
        seq = x.shape[1]
        total_cols = cols * group
        tail = cols % TILE
        items = 3 * CHUNKS * 2 * layers
        cos, sin = rope_tables(seq)
        any_spec = pl.BlockSpec(memory_space=pl.ANY)
        vmem_spec = pl.BlockSpec(memory_space=pltpu.VMEM)
        bf16, f32 = jnp.bfloat16, jnp.float32
        dma = pltpu.SemaphoreType.DMA
        out = pl.pallas_call(
            functools.partial(kernel, groups, group),
            out_shape=(
                jax.ShapeDtypeStruct(x.shape, bf16),
                jax.ShapeDtypeStruct((layers, 1, seq, HEAD_DIM), bf16),
                jax.ShapeDtypeStruct((layers, 1, seq, HEAD_DIM), bf16),
                jax.ShapeDtypeStruct((layers, group, cols, width), bf16),
                jax.ShapeDtypeStruct((layers, group, out_rows, width), bf16),
            ),
            in_specs=[any_spec, vmem_spec, vmem_spec, vmem_spec, any_spec, any_spec],
            out_specs=[any_spec] * 5,
            scratch_shapes=[
                pltpu.VMEM((seq, width), bf16),
                pltpu.VMEM((seq, width), f32),
                pltpu.VMEM((seq, total_cols), bf16),
                pltpu.VMEM((seq, HEAD_DIM), bf16),
                pltpu.VMEM((seq, HEAD_DIM), bf16),
                pltpu.VMEM((2, TILE, width), bf16),
                pltpu.VMEM((tail, width), bf16),
                pltpu.VMEM((2, out_rows, TILE), bf16),
                dma((items,)),
                dma((items,)),
                dma((2 * layers, 3)),
                dma((2 * layers, 5)),
                dma((2 * layers, 9)),
                dma((2 * layers, 5)),
                dma((2,)),
                dma((2,)),
                dma,
                dma((2,)),
            ],
            compiler_params=pltpu.CompilerParams(
                collective_id=0, has_side_effects=True, vmem_limit_bytes=67_043_328
            ),
        )(x, gain, cos, sin, w_in, w_out)
        return out[:3]

    return jax.shard_map(
        device_program,
        mesh=mesh,
        in_specs=(P(batch_axes, None, None), P(None, None), P(None, None, "fsdp"), P(None, "fsdp", None)),
        out_specs=(P(batch_axes, None, None), P(None, batch_axes, None, None), P(None, batch_axes, None, None)),
        check_vma=False,
    )
```

```python
import functools

import jax
import jax.numpy as jnp
import numpy as np
from jax import lax
from jax.experimental import pallas as pl
from jax.experimental.pallas import tpu as pltpu
from jax.sharding import PartitionSpec as P

HEAD_DIM = 256
ROPE_BASE = 10000.0
NORM_EPS = 1e-6
MESH = pl.DeviceIdType.MESH
TILE = 512
CHUNKS = 4
AHEAD = 4


def rope_tables(seq_len):
    half = HEAD_DIM // 2
    angle = np.arange(seq_len)[:, None] * ROPE_BASE ** (-np.arange(half) / half)
    return np.cos(angle).astype(np.float32), np.sin(angle).astype(np.float32)


def part_rows(rows):
    step = 8 * CHUNKS
    outer = round(rows / (3 * step)) * step
    return outer, rows - 2 * outer


def aligned(value, step):
    return pl.multiple_of(value, step)


def loop(lo, hi, body):
    lax.fori_loop(lo, hi, lambda i, c: (body(i), c)[1], 0)


def kernel(
    groups, group, x_ref, gain_ref, cos_ref, sin_ref, w_in_ref, w_out_ref,
    y_ref, k_ref, v_ref, g_in, g_out,
    h, acc, proj, kbuf, vbuf, wbuf, wtail, obuf,
    rx, rm, rp, rd, send, sd, wsem, tsem, ysem, kvsem,
):
    layers, cols, width = w_in_ref.shape
    out_rows = w_out_ref.shape[1]
    seq = x_ref.shape[1]
    rows_total = out_rows * group
    ff = cols * group - rows_total - 2 * HEAD_DIM
    q_cols = rows_total - ff
    heads = q_cols // HEAD_DIM
    chips = group // 2
    n_full = cols // TILE
    rest = (cols - n_full * TILE) // 128 * 128
    edge = cols - n_full * TILE - rest
    half = HEAD_DIM // 2
    items = 3 * CHUNKS
    total = items * 2 * layers

    dp = lax.axis_index("dp")
    me = lax.axis_index("fsdp")
    chip, core = lax.div(me, 2), lax.rem(me, 2)
    side = lax.rem(dp, 2)

    def dev(chip_off, other_core=0):
        c = core if isinstance(other_core, int) and other_core == 0 else lax.rem(core + other_core, 2)
        return 2 * lax.rem(chip + chip_off + chips, chips) + c

    right, left, far = dev(1), dev(-1), dev(2)
    sib = 2 * chip + (1 - core)
    to_right, to_left = {"dp": dp, "fsdp": right}, {"dp": dp, "fsdp": left}
    to_pair = {"dp": dp + 1 - 2 * side, "fsdp": me}
    to_sib = {"dp": dp, "fsdp": sib}

    barrier = pltpu.get_barrier_semaphore()
    for target in (to_right, to_left, to_pair, to_sib):
        pl.semaphore_signal(barrier, inc=1, device_id=target, device_id_type=MESH)
    pl.semaphore_wait(barrier, 4)

    kinds = []
    for own, land, rows in ((w_in_ref, g_in, cols), (w_out_ref, g_out, out_rows)):
        outer, middle = part_rows(rows)
        kinds.append((own, land, outer, middle))

    def part_at(kind, part):
        _, _, outer, middle = kinds[kind]
        if part == 1:
            return outer, middle
        where = side if part == 0 else 1 - side
        return where * (outer + middle), outer

    def region(kind, part, k):
        start, rows = part_at(kind, part)
        return aligned(start + k * (rows // CHUNKS), 8), rows // CHUNKS

    def remote(kind, src, slot, layer, off, rows, ssem, rsem, target):
        _, land, _, _ = kinds[kind]
        source = src.at[layer] if slot is None else src.at[layer, slot]
        return pltpu.make_async_remote_copy(
            src_ref=source.at[pl.ds(off, rows)],
            dst_ref=land.at[layer, me if slot is None else slot, pl.ds(off, rows)],
            send_sem=ssem, recv_sem=rsem, device_id=target, device_id_type=MESH,
        )

    def arrival(kind, layer, slot, off, rows, rsem):
        _, land, _, _ = kinds[kind]
        ref = land.at[layer, slot, pl.ds(off, rows)]
        return pltpu.make_async_remote_copy(
            src_ref=ref, dst_ref=ref, send_sem=sd.at[0], recv_sem=rsem,
            device_id=to_sib, device_id_type=MESH,
        )

    def send_x(g):
        w, i = lax.div(g, items), lax.rem(g, items)
        layer = lax.div(w, 2)
        k = lax.rem(i, CHUNKS)
        for kind in range(2):
            own, land, _, _ = kinds[kind]

            @pl.when(lax.rem(w, 2) == kind)
            def _():
                for stage in range(3):
                    @pl.when((lax.div(i, CHUNKS) == stage))
                    def _():
                        for way, (target, rsem) in enumerate(((to_right, rx), (to_left, rm))):
                            ssem = send.at[w, 3 * way + stage]
                            if stage < 2:
                                off, rows = region(kind, stage, k)
                                remote(kind, own, None, layer, off, rows, ssem, rsem.at[g], target).start()
                            else:
                                off, rows = region(kind, way, k)
                                slot = left if way == 0 else right
                                remote(kind, land, slot, layer, off, rows, ssem, rsem.at[g], target).start()

    def tick(g):
        w, i = lax.div(g, items), lax.rem(g, items)
        layer = lax.div(w, 2)
        k = lax.rem(i, CHUNKS)
        for kind in range(2):
            _, land, _, _ = kinds[kind]

            @pl.when(lax.rem(w, 2) == kind)
            def _():
                for stage in range(3):
                    @pl.when((lax.div(i, CHUNKS) == stage))
                    def _():
                        for way, rsem in enumerate((rx, rm)):
                            slot = far if stage == 2 else (left if way == 0 else right)
                            off, rows = region(kind, way if stage == 2 else stage, k)
                            arrival(kind, layer, slot, off, rows, rsem.at[g]).wait_recv()
                        off, rows = region(kind, 0, k)
                        if stage == 0:
                            for n, slot in enumerate((left, right)):
                                remote(kind, land, slot, layer, off, rows, send.at[w, 6 + n], rp.at[w, n], to_pair).start()
                        if stage == 2:
                            remote(kind, land, far, layer, off, rows, send.at[w, 8], rp.at[w, 2], to_pair).start()

        @pl.when(g + AHEAD < total)
        def _():
            send_x(g + AHEAD)

    def ticks(lo, hi):
        loop(jnp.minimum(lo, total), jnp.minimum(hi, total), tick)

    def take_pair(kind, layer, n):
        off, rows = part_at(kind, 2)
        off = aligned(off, 8)
        slot = (left, right, far)[n]
        arrival(kind, layer, slot, off, rows, rp.at[2 * layer + kind, n]).wait_recv()

    def sib_rows(kind, n):
        _, _, outer, middle = kinds[kind]
        if n < 3:
            return 0, 2 * outer + middle
        if n == 3:
            return aligned(side * outer, 8), outer + middle
        off, rows = part_at(kind, 2)
        return aligned(off, 8), rows

    def sib_send(kind, layer, n):
        own, land, outer, middle = kinds[kind]
        w = 2 * layer + kind
        src, slot = (own, None) if n == 0 else (land, (None, left, right, far, far)[n])
        off, rows = sib_rows(kind, n)
        remote(kind, src, slot, layer, off, rows, sd.at[w, n], rd.at[w, n], to_sib).start()

    def sib_slot(n):
        return (sib, dev(-1, 1), dev(1, 1), dev(2, 1), dev(2, 1))[n]

    def take_sib(kind, layer, n):
        off, rows = sib_rows(kind, n)
        ref = kinds[kind][1].at[layer, sib_slot(n), pl.ds(off, rows)]
        pltpu.make_async_remote_copy(
            src_ref=ref, dst_ref=ref, send_sem=sd.at[2 * layer + kind, n], recv_sem=rd.at[2 * layer + kind, n],
            device_id=to_sib, device_id_type=MESH,
        ).wait_recv()

    def shard_at(s):
        off = jnp.where(s < 2, 0, jnp.where(s >= 6, 2, jnp.where(lax.rem(s, 2) == 0, -1, 1)))
        flip = jnp.where((s == 1) | (s == 4) | (s == 5) | (s == 7), 1, 0)
        return 2 * lax.rem(chip + off + chips, chips) + lax.rem(core + flip, 2)

    def primed(s):
        return (s == 1) | (s == 3) | (s == 5)

    def normalise(layer):
        gains = gain_ref[...].astype(jnp.float32)
        chosen = lax.broadcasted_iota(jnp.int32, gains.shape, 0) == layer
        gain = jnp.sum(jnp.where(chosen, gains, 0.0), axis=0, keepdims=True)

        def block(b):
            rows = pl.ds(aligned(b * 128, 128), 128)
            hidden = acc[rows, :].astype(jnp.bfloat16).astype(jnp.float32)
            acc[rows, :] = hidden
            centred = hidden - jnp.mean(hidden, axis=-1, keepdims=True)
            variance = jnp.mean(centred * centred, axis=-1, keepdims=True)
            h[rows, :] = (centred * lax.rsqrt(variance + NORM_EPS) * gain).astype(jnp.bfloat16)

        loop(0, seq // 128, block)

    def in_shard(layer, s):
        d = shard_at(s)
        odd = lax.rem(d, 2)
        first = odd * edge
        base = aligned(d * cols + first, 128)

        def fetch(start, rows, target, sem, s=s, d=d):
            @pl.when(s == 0)
            def _():
                pltpu.make_async_copy(w_in_ref.at[layer, pl.ds(aligned(start, 8), rows)], target, sem).start()

            @pl.when(s > 0)
            def _():
                pltpu.make_async_copy(g_in.at[layer, d, pl.ds(aligned(start, 8), rows)], target, sem).start()

        def product(weights):
            return lax.dot_general(
                h[...], weights, (((1,), (1,)), ((), ())), preferred_element_type=jnp.float32
            ).astype(jnp.bfloat16)

        @pl.when(jnp.logical_not(primed(s)))
        def _():
            fetch(first, TILE, wbuf.at[0], wsem.at[0])

        fetch(first + n_full * TILE, rest, wtail.at[pl.ds(0, rest)], tsem.at[0])
        fetch((1 - odd) * (n_full * TILE + rest), edge, wtail.at[pl.ds(rest, edge)], tsem.at[1])

        def full(j):
            slot = lax.rem(j, 2)

            @pl.when(j + 1 < n_full)
            def _():
                fetch(first + (j + 1) * TILE, TILE, wbuf.at[1 - slot], wsem.at[1 - slot])

            @pl.when((j + 1 == n_full) & primed(s + 1))
            def _():
                ahead = shard_at(s + 1)
                fetch(lax.rem(ahead, 2) * edge, TILE, wbuf.at[n_full % 2], wsem.at[n_full % 2], s + 1, ahead)

            pltpu.make_async_copy(g_in.at[0, 0, pl.ds(0, TILE)], wbuf.at[slot], wsem.at[slot]).wait()
            proj[:, pl.ds(aligned(base + j * TILE, 128), TILE)] = product(wbuf[slot])

        loop(0, n_full, full)
        pltpu.make_async_copy(g_in.at[0, 0, pl.ds(0, rest)], wtail.at[pl.ds(0, rest)], tsem.at[0]).wait()
        pltpu.make_async_copy(g_in.at[0, 0, pl.ds(0, edge)], wtail.at[pl.ds(rest, edge)], tsem.at[1]).wait()
        last = product(wtail[...])
        proj[:, pl.ds(aligned(base + n_full * TILE, 128), rest)] = last[:, :rest]
        edges = proj.at[:, pl.ds(aligned(jnp.where(odd == 1, base - 128, base + n_full * TILE + rest), 128), 128)]

        @pl.when(odd == 0)
        def _():
            edges[:, :edge] = last[:, rest:]

        @pl.when(odd == 1)
        def _():
            edges[:, 128 - edge:] = last[:, rest:]

    def rotate(a, rows):
        cos, sin = cos_ref[rows, :], sin_ref[rows, :]
        first, second = a[:, :half], a[:, half:]
        return jnp.concatenate([first * cos - second * sin, second * cos + first * sin], axis=-1)

    q_block = 256

    def keys(layer):
        def block(b):
            rows = pl.ds(aligned(b * q_block, q_block), q_block)
            key = proj[rows, q_cols:q_cols + HEAD_DIM].astype(jnp.float32)
            kbuf[rows, :] = rotate(key, rows).astype(jnp.bfloat16)
            vbuf[rows, :] = proj[rows, q_cols + HEAD_DIM:q_cols + 2 * HEAD_DIM]

        loop(0, seq // q_block, block)
        pltpu.make_async_copy(kbuf, k_ref.at[layer, 0], kvsem.at[0]).start()
        pltpu.make_async_copy(vbuf, v_ref.at[layer, 0], kvsem.at[1]).start()

    blocks = seq // q_block
    shift_cols = 2 * HEAD_DIM

    def attend(t):
        two = heads // 2 - 1 - lax.div(t, blocks)
        b = lax.rem(t, blocks)
        rows = pl.ds(aligned(b * q_block, q_block), q_block)
        q = proj[rows, pl.ds(aligned(two * 2 * HEAD_DIM, 2 * HEAD_DIM), 2 * HEAD_DIM)].astype(jnp.float32)
        q = jnp.concatenate([rotate(q[:, :HEAD_DIM], rows), rotate(q[:, HEAD_DIM:], rows)], axis=0)
        q = (q * HEAD_DIM ** -0.5).astype(jnp.bfloat16)
        for n in range(blocks):
            @pl.when(b == n)
            def _():
                seen = (n + 1) * q_block
                s = lax.dot_general(q, kbuf[:seen, :], (((1,), (1,)), ((), ())), preferred_element_type=jnp.float32)
                own = s[:, n * q_block:]
                row = lax.broadcasted_iota(jnp.int32, own.shape, 0) & (q_block - 1)
                own = jnp.where(row >= lax.broadcasted_iota(jnp.int32, own.shape, 1), own, -1e30)
                s = own if n == 0 else jnp.concatenate([s[:, :n * q_block], own], axis=1)
                e = jnp.exp(s - jnp.max(s, axis=-1, keepdims=True))
                o = jnp.dot(e.astype(jnp.bfloat16), vbuf[:seen, :], preferred_element_type=jnp.float32)
                o = (o / jnp.sum(e, axis=-1, keepdims=True)).astype(jnp.bfloat16)
                place = pl.ds(aligned(two * 2 * HEAD_DIM + shift_cols, 2 * HEAD_DIM), 2 * HEAD_DIM)
                proj[rows, place] = jnp.concatenate([o[:q_block], o[q_block:]], axis=1)

    gate0 = q_cols + 2 * HEAD_DIM
    up0 = gate0 + ff

    def gated(t):
        def block(b):
            rows = pl.ds(aligned(b * 256, 256), 256)
            gate_cols = pl.ds(aligned(gate0 + t * TILE, 128), TILE)
            gate = proj[rows, gate_cols].astype(jnp.float32)
            up = proj[rows, pl.ds(aligned(up0 + t * TILE, 128), TILE)].astype(jnp.float32)
            proj[rows, gate_cols] = (jax.nn.silu(gate) * up).astype(jnp.bfloat16)

        loop(0, seq // 256, block)

    n_out = width // TILE

    def out_shard(layer, s):
        d = shard_at(s)

        def fetch(n, slot, s=s, d=d):
            window = pl.ds(aligned(n * TILE, TILE), TILE)
            target = obuf.at[slot]

            @pl.when(s == 0)
            def _():
                pltpu.make_async_copy(w_out_ref.at[layer, :, window], target, wsem.at[slot]).start()

            @pl.when(s > 0)
            def _():
                pltpu.make_async_copy(g_out.at[layer, d, :, window], target, wsem.at[slot]).start()

        @pl.when(jnp.logical_not(primed(s)))
        def _():
            fetch(0, 0)

        left_cols = pl.ds(aligned(shift_cols + d * out_rows, 128), out_rows)

        def tile(n):
            slot = lax.rem(n, 2)

            @pl.when(n + 1 < n_out)
            def _():
                fetch(n + 1, 1 - slot)

            @pl.when((n + 1 == n_out) & primed(s + 1))
            def _():
                fetch(0, n_out % 2, s + 1, shard_at(s + 1))

            pltpu.make_async_copy(g_out.at[0, 0, :, pl.ds(0, TILE)], obuf.at[slot], wsem.at[slot]).wait()
            window = pl.ds(aligned(n * TILE, TILE), TILE)
            acc[:, window] += jnp.dot(proj[:, left_cols], obuf[slot], preferred_element_type=jnp.float32)

            @pl.when((layer == layers - 1) & (s == 7))
            def _():
                h[:, window] = acc[:, window].astype(jnp.bfloat16)
                pltpu.make_async_copy(h.at[:, window], y_ref.at[0, :, window], ysem).start()

        loop(0, n_out, tile)

    loop(0, AHEAD, send_x)
    copy = pltpu.make_async_copy(x_ref.at[0], h, ysem)
    copy.start()
    copy.wait()

    def widen(b):
        rows = pl.ds(aligned(b * 128, 128), 128)
        acc[rows, :] = h[rows, :].astype(jnp.float32)

    loop(0, seq // 128, widen)

    def layer_step(layer):
        g0 = 2 * items * layer
        sib_send(0, layer, 0)
        sib_send(1, layer, 0)
        normalise(layer)

        def run_ticks(s, start, ends):
            lo, hi = start, ends[0]
            for n in range(1, len(ends)):
                lo = jnp.where(s == n, ends[n - 1], lo)
                hi = jnp.where(s == n, ends[n], hi)
            ticks(g0 + lo, g0 + hi)

        def in_step(s):
            n = 3 * CHUNKS
            ends = (1, 2, 10, 11, 12, 13, 14, 15)
            run_ticks(s, 1, ends)

            @pl.when(s == 0)
            def _():
                take_sib(0, layer, 0)

            @pl.when(s == 2)
            def _():
                for n in (0, 1):
                    take_pair(0, layer, n)
                    sib_send(0, layer, n + 1)

            for first, at in ((1, 4), (3, 7)):
                @pl.when(s == at)
                def _():
                    take_sib(0, layer, first)
                    take_sib(0, layer, first + 1)

            @pl.when(s == 4)
            def _():
                sib_send(0, layer, 3)

            @pl.when(s == 6)
            def _():
                take_pair(0, layer, 2)
                sib_send(0, layer, 4)

            in_shard(layer, s)

        loop(0, 8, in_step)
        keys(layer)

        def attend_step(t):
            @pl.when(lax.rem(t, 4) == 2)
            def _():
                n = g0 + 15 + lax.div(t, 4)
                ticks(n, n + 1)
            attend(t)

        loop(0, heads // 2 * blocks, attend_step)

        def gated_step(t):
            gated(t)

        loop(0, ff // TILE, gated_step)

        def out_step(s):
            n = 6 * CHUNKS
            run_ticks(s, 19, (21, 22, 22, 23, 24, 24, 25, 25))

            @pl.when(s == 0)
            def _():
                take_sib(1, layer, 0)

            @pl.when(s == 2)
            def _():
                for n in (0, 1):
                    take_pair(1, layer, n)
                    sib_send(1, layer, n + 1)

            for first, at in ((1, 4), (3, 7)):
                @pl.when(s == at)
                def _():
                    take_sib(1, layer, first)
                    take_sib(1, layer, first + 1)

            @pl.when(s == 5)
            def _():
                sib_send(1, layer, 3)

            @pl.when(s == 6)
            def _():
                take_pair(1, layer, 2)
                sib_send(1, layer, 4)

            out_shard(layer, s)

        loop(0, 8, out_step)
        pltpu.make_async_copy(kbuf, k_ref.at[layer, 0], kvsem.at[0]).wait()
        pltpu.make_async_copy(vbuf, v_ref.at[layer, 0], kvsem.at[1]).wait()

    tick(0)
    loop(0, layers, layer_step)

    copy = pltpu.make_async_copy(h, y_ref.at[0], ysem)

    def drain(layer):
        for kind in range(2):
            _, land, outer, middle = kinds[kind]
            w = 2 * layer + kind
            for n in range(9):
                rows = middle if n in (1, 4, 5) else outer
                ref = land.at[layer, 0, pl.ds(0, rows)]
                pltpu.make_async_remote_copy(
                    src_ref=ref, dst_ref=ref, send_sem=send.at[w, n], recv_sem=rx.at[0],
                    device_id=to_sib, device_id_type=MESH,
                ).wait_send()
            for n in range(5):
                ref = land.at[layer, 0, pl.ds(0, sib_rows(kind, n)[1])]
                pltpu.make_async_remote_copy(
                    src_ref=ref, dst_ref=ref, send_sem=sd.at[w, n], recv_sem=rx.at[0],
                    device_id=to_sib, device_id_type=MESH,
                ).wait_send()

    loop(0, layers, drain)
    copy.wait()


def solution(mesh):
    batch_axes = ("dp", "fsdp")
    groups, group = mesh.shape["dp"], mesh.shape["fsdp"]

    def device_program(x, gain, w_in, w_out):
        w_in = jnp.swapaxes(w_in, 1, 2)
        layers, cols, width = w_in.shape
        out_rows = w_out.shape[1]
        seq = x.shape[1]
        total_cols = cols * group
        tail = cols % TILE
        items = 3 * CHUNKS * 2 * layers
        cos, sin = rope_tables(seq)
        any_spec = pl.BlockSpec(memory_space=pl.ANY)
        vmem_spec = pl.BlockSpec(memory_space=pltpu.VMEM)
        bf16, f32 = jnp.bfloat16, jnp.float32
        dma = pltpu.SemaphoreType.DMA
        out = pl.pallas_call(
            functools.partial(kernel, groups, group),
            out_shape=(
                jax.ShapeDtypeStruct(x.shape, bf16),
                jax.ShapeDtypeStruct((layers, 1, seq, HEAD_DIM), bf16),
                jax.ShapeDtypeStruct((layers, 1, seq, HEAD_DIM), bf16),
                jax.ShapeDtypeStruct((layers, group, cols, width), bf16),
                jax.ShapeDtypeStruct((layers, group, out_rows, width), bf16),
            ),
            in_specs=[any_spec, vmem_spec, vmem_spec, vmem_spec, any_spec, any_spec],
            out_specs=[any_spec] * 5,
            scratch_shapes=[
                pltpu.VMEM((seq, width), bf16),
                pltpu.VMEM((seq, width), f32),
                pltpu.VMEM((seq, total_cols), bf16),
                pltpu.VMEM((seq, HEAD_DIM), bf16),
                pltpu.VMEM((seq, HEAD_DIM), bf16),
                pltpu.VMEM((2, TILE, width), bf16),
                pltpu.VMEM((tail, width), bf16),
                pltpu.VMEM((2, out_rows, TILE), bf16),
                dma((items,)),
                dma((items,)),
                dma((2 * layers, 3)),
                dma((2 * layers, 5)),
                dma((2 * layers, 9)),
                dma((2 * layers, 5)),
                dma((2,)),
                dma((2,)),
                dma,
                dma((2,)),
            ],
            compiler_params=pltpu.CompilerParams(
                collective_id=0, has_side_effects=True, vmem_limit_bytes=67_043_328
            ),
        )(x, gain, cos, sin, w_in, w_out)
        return out[:3]

    return jax.shard_map(
        device_program,
        mesh=mesh,
        in_specs=(P(batch_axes, None, None), P(None, None), P(None, None, "fsdp"), P(None, "fsdp", None)),
        out_specs=(P(batch_axes, None, None), P(None, batch_axes, None, None), P(None, batch_axes, None, None)),
        check_vma=False,
    )
```
